32 devices in a mesh: dp: 16 (over z, y, core), group: 2 (over x).
Axes of the slice: x: 2, y: 2, z: 4, core: 2. Of those that a mesh axis runs over, the one named last changes fastest.
Arguments:
- rewards: float32 [512, 4096], P(('dp', 'group')), may hold values from -6 to 6
- values: float32 [512, 4096], P(('dp', 'group')), may hold values from -6 to 6
- horizon: float32 [512], P(('dp', 'group')), may hold values from 16 to 32768
- lengths: int32 [512], P(('dp', 'group')), may hold values from 1 to 4096
- assignment: int32 [16, 1024], P('dp', 'group'), may hold values from 0 to 1023, as said below
Outputs:
- returns: float32 [512, 4096], P(('dp', 'group'))
- train_adv: float32 [16384, 128], P(('dp', 'group'))
The draws below stay inside these ranges and needn't reach their ends.
Inputs may be any that keep to these rules, and one draw needn't show every extreme that they name: Each row of assignment names each of the 1024 blocks of its index of dp once; the slots held by one device take at most 512 blocks from the sequences of any one device of its group, and that most is reached in every row.
All inputs are finite; a program needn't handle non-finite values.
Results may differ from the reference program's by a relative error of at most 0.0001.
Values sent between devices are 32-bit elements; how exact they have to be, the bound alone decides.
No kernel may reach another device: no remote copies, remote signals or barrier semaphores. Data moves between devices by JAX's collectives and lax.ppermute only.
A program may use at most 64 MiB of HBM per device.

```python
import math
import jax
import jax.numpy as jnp
from jax import lax

LEN = 4096
BLK = 128
SEQS = 512
GBLK = 1024
N_DP = 16
N_GROUP = 2


def assign_row(key):
    per_dev = GBLK // N_GROUP
    quota = per_dev // N_GROUP
    key_a, key_b, key_p, key_n = jax.random.split(key, 4)
    first = jax.random.randint(key_a, (), 0, N_GROUP, dtype=jnp.int32)
    second = (first + jax.random.randint(key_b, (), 1, N_GROUP, dtype=jnp.int32)) % N_GROUP
    source = jnp.arange(N_GROUP, dtype=jnp.int32)[:, None]
    target = jnp.arange(N_GROUP, dtype=jnp.int32)[None, :]
    plus = (target == (source + first) % N_GROUP).astype(jnp.int32)
    minus = (target == (source + second) % N_GROUP).astype(jnp.int32)
    counts = quota + quota * (plus - minus)
    ends = jnp.cumsum(counts, axis=1)
    place = jnp.arange(per_dev, dtype=jnp.int32)
    dest_of = jnp.sum((place[None, :, None] >= ends[:, None, :]).astype(jnp.int32), axis=2)
    perm_keys = jax.random.split(key_p, N_GROUP)
    perms = jax.vmap(lambda k: jax.random.permutation(k, per_dev))(perm_keys).astype(jnp.int32)
    block_ids = source * per_dev + perms
    dest_block = jnp.zeros((GBLK,), jnp.int32).at[block_ids.reshape(-1)].set(dest_of.reshape(-1))
    noise = jax.random.permutation(key_n, GBLK).astype(jnp.int32)
    order_keys = dest_block * GBLK + noise
    return jnp.argsort(order_keys, stable=True).astype(jnp.int32)


def draw_assignment(key, part):
    keys = jax.random.split(jax.random.fold_in(key, 7), N_DP)
    return jax.vmap(assign_row)(keys)


def plant(drawn, own_key, low, largest):
    shape = drawn.shape
    spot = [jax.random.randint(jax.random.fold_in(own_key, axis), (), 0, shape[axis]) for axis in range(len(shape))]
    drawn = drawn.at[tuple(spot)].set(low)
    longest = shape.index(max(shape))
    spot[longest] = (spot[longest] + 1) % shape[longest]
    return drawn.at[tuple(spot)].set(largest)


def level_of(rng, shape, pieces, low, high):
    loudness = 1.0
    for axis_at, shards_of in pieces:
        heights = jax.random.uniform(jax.random.fold_in(jax.random.fold_in(rng, 6), axis_at), (shards_of,), jnp.float32, low / len(pieces), high / len(pieces))
        loudness = loudness * jnp.repeat(jnp.exp(heights), shape[axis_at] // shards_of).reshape((-1,) + (1,) * (len(shape) - 1 - axis_at))
    return loudness


def gaussian(stream_key, dims, scale, most, cuts=(), held_as=jnp.bfloat16):
    values = scale * jax.random.normal(stream_key, dims, jnp.float32)
    if cuts:
        values = values * level_of(stream_key, dims, cuts, -0.22, 0.18)
    return jnp.clip(values, -most, most).astype(held_as)


def setup_inputs(seed: int = 0) -> dict:
    splits = jax.random.split(jax.random.key(seed), 6)
    rewards = gaussian(splits[0], (SEQS, LEN), 1.0, 6.0, ((0, 32),), jnp.float32)
    values = gaussian(splits[1], (SEQS, LEN), 1.0, 6.0, ((0, 32),), jnp.float32)
    horizon = jnp.clip(jnp.exp(math.log(32768.0) - 7.624619 * jax.random.uniform(splits[2], (SEQS,), jnp.float32) ** level_of(splits[2], (SEQS,), ((0, 32),), -0.2, 0.2)), 16.0, 32768.0)
    lengths = plant(jax.random.randint(splits[3], (SEQS,), 1, LEN + 1), jax.random.fold_in(splits[3], 1), 1, LEN).astype(jnp.int32)
    assignment = draw_assignment(jax.random.fold_in(splits[5], 71), 0)
    return {"rewards": rewards, "values": values, "horizon": horizon, "lengths": lengths, "assignment": assignment}


trace_decay = 0.998
epsilon = 1e-05

def reference(rewards, values, horizon, lengths, assignment):
    gamma = 1.0 - 1.0 / horizon
    coeff = gamma * trace_decay
    position = jnp.arange(LEN, dtype=jnp.int32)
    inside = position[None, :] < lengths[:, None]
    follows = position[None, :] + 1 < lengths[:, None]
    shifted = jnp.concatenate([values[:, 1:], jnp.zeros((SEQS, 1), values.dtype)], axis=1)
    upcoming = jnp.where(follows, shifted, 0.0)
    deltas = jnp.where(inside, rewards + gamma[:, None] * upcoming - values, 0.0)

    def backward(carry, column):
        value_now = column + coeff * carry
        return (value_now, value_now)
    _, advantage = lax.scan(backward, jnp.zeros((SEQS,), rewards.dtype), deltas.T, reverse=True)
    advantage = advantage.T
    returns = jnp.where(inside, advantage + values, 0.0)
    weight = inside.astype(rewards.dtype)
    counted = jnp.sum(weight)
    center = jnp.sum(advantage * weight) / counted
    spread = jnp.sum(weight * (advantage - center) ** 2)
    scale = lax.rsqrt(spread / counted + epsilon)
    whitened = jnp.where(inside, (advantage - center) * scale, 0.0)
    blocks = whitened.reshape(N_DP, GBLK, BLK)
    chosen = jnp.take_along_axis(blocks, assignment.astype(jnp.int32)[:, :, None], axis=1)
    return (returns, chosen.reshape(N_DP * GBLK, BLK))
```

```python
import functools

import jax
import jax.numpy as jnp
from jax import lax
from jax.experimental import pallas as pl
from jax.experimental.pallas import tpu as pltpu
from jax.sharding import PartitionSpec as P

BLK = 128
trace_decay = 0.998
epsilon = 1e-05
OUTSIDE = 1e30
LANES = 128
ROWS = 8


def column(ref, first, dtype):
    row = lax.broadcasted_iota(jnp.int32, (ROWS, LANES), 0)
    out = jnp.zeros((ROWS, LANES), dtype)
    for k in range(ROWS):
        out = jnp.where(row == k, ref[first + k], out)
    return out[:, :1]


def advantage_kernel(me_ref, horizon_ref, lengths_ref, rewards_ref, values_ref, returns_ref, blocks_ref, stats_ref):
    seqs, local = rewards_ref.shape
    per_row = local // BLK
    position = lax.broadcasted_iota(jnp.int32, (ROWS, local), 1)
    parts = []
    for first in range(0, seqs, ROWS):
        rows = pl.ds(first, ROWS)
        length = column(lengths_ref, first, jnp.int32)
        discount = 1.0 - 1.0 / column(horizon_ref, first, jnp.float32)
        rewards = rewards_ref[rows, :]
        values = values_ref[rows, :]
        inside = position < length
        shifted = pltpu.roll(values, local - 1, 1)
        upcoming = jnp.where(position + 1 < length, shifted, 0.0)
        total = jnp.where(inside, rewards + discount * upcoming - values, 0.0)
        power = discount * trace_decay
        step = 1
        while step < local:
            ahead = pltpu.roll(total, local - step, 1)
            total = total + power * jnp.where(position < local - step, ahead, 0.0)
            power = power * power
            step *= 2
        returns_ref[rows, :] = jnp.where(inside, total + values, 0.0)
        marked = jnp.where(inside, total, OUTSIDE)
        for block in range(per_row):
            blocks_ref[pl.ds(first * per_row + block, ROWS, stride=per_row), :] = marked[:, block * BLK : (block + 1) * BLK]
        parts.append((inside, total, jnp.sum(length.astype(jnp.float32))))
    count = sum(part[2] for part in parts)
    mean = sum(jnp.sum(part[1]) for part in parts) / count
    spread = sum(jnp.sum(jnp.where(part[0], (part[1] - mean) ** 2, 0.0)) for part in parts)
    wide = stats_ref.shape[1]
    row = lax.broadcasted_iota(jnp.int32, (ROWS, wide), 0)
    mine = lax.broadcasted_iota(jnp.int32, (ROWS, wide), 1) == me_ref[0]
    stats = jnp.where(row == 0, count, jnp.where(row == 1, mean, jnp.where(row == 2, spread, 0.0)))
    stats_ref[...] = jnp.where(mine, stats, 0.0)


def place_kernel(members, me_ref, wanted_ref, stats_ref, *refs):
    sources, (out_ref, pool_ref) = refs[:members], refs[members:]
    slots = out_ref.shape[0]
    share = sources[0].shape[0]
    group = me_ref[1]
    for k in range(members):
        owner = lax.rem(group + k, members)
        pool_ref[pl.ds(pl.multiple_of(owner * share, share), share), :] = sources[k][...]

    def move(i, carry):
        for k in range(ROWS):
            slot = i * ROWS + k
            out_ref[pl.ds(slot, 1), :] = pool_ref[pl.ds(wanted_ref[0, slot], 1), :]
        return carry

    lax.fori_loop(0, slots // ROWS, move, 0)
    count, mean, spread = stats_ref[0:1, :], stats_ref[1:2, :], stats_ref[2:3, :]
    total = jnp.sum(count)
    center = jnp.sum(count * mean) / total
    deviation = jnp.sum(spread + count * (mean - center) ** 2)
    scale = lax.rsqrt(jnp.full((1, LANES), deviation / total + epsilon, jnp.float32))
    moved = out_ref[...]
    out_ref[...] = jnp.where(moved == OUTSIDE, 0.0, (moved - center) * scale)


def merged(mine, other):
    return jnp.where(other[:1] > 0.0, other, mine)


def spread_all(stats, axis, size):
    reach = 1
    while reach < size:
        pairs = [(i, (i + reach) % size) for i in range(size)]
        stats = merged(stats, lax.ppermute(stats, axis, pairs))
        reach *= 2
    return stats


def body(rewards, values, horizon, lengths, assignment):
    seqs, local = rewards.shape
    n_dp, n_group = lax.axis_size("dp"), lax.axis_size("group")
    slots = assignment.shape[-1]
    wide = -(-n_dp * n_group // LANES) * LANES
    group = lax.axis_index("group")
    me = jnp.stack([lax.axis_index("dp") * n_group + group, group]).astype(jnp.int32)
    smem = pl.BlockSpec(memory_space=pltpu.SMEM)
    vmem = pl.BlockSpec(memory_space=pltpu.VMEM)
    f32 = jnp.float32
    returns, blocks, stats = pl.pallas_call(
        advantage_kernel,
        out_shape=(
            jax.ShapeDtypeStruct((seqs, local), f32),
            jax.ShapeDtypeStruct((seqs * local // BLK, BLK), f32),
            jax.ShapeDtypeStruct((ROWS, wide), f32),
        ),
        in_specs=[smem, smem, smem, vmem, vmem],
        out_specs=(vmem, vmem, vmem),
        compiler_params=pltpu.CompilerParams(vmem_limit_bytes=16 << 20),
    )(me, horizon, lengths, rewards, values)
    sources = [blocks]
    for k in range(1, n_group):
        sources.append(lax.ppermute(blocks, "group", [((i + k) % n_group, i) for i in range(n_group)]))
    stats = spread_all(stats, "group", n_group)
    stats = spread_all(stats, "dp", n_dp)
    train = pl.pallas_call(
        functools.partial(place_kernel, n_group),
        out_shape=jax.ShapeDtypeStruct((slots, BLK), f32),
        in_specs=[smem, smem, vmem] + [vmem] * n_group,
        out_specs=vmem,
        scratch_shapes=[pltpu.VMEM((n_group * blocks.shape[0], BLK), f32)],
        compiler_params=pltpu.CompilerParams(vmem_limit_bytes=16 << 20),
    )(me, assignment, stats, *sources)
    return (returns, train)


def solution(mesh):
    in_specs = (
        P(("dp", "group"), None),
        P(("dp", "group"), None),
        P(("dp", "group")),
        P(("dp", "group")),
        P("dp", "group"),
    )
    out_specs = (P(("dp", "group"), None), P(("dp", "group"), None))
    return jax.shard_map(body, mesh=mesh, in_specs=in_specs, out_specs=out_specs, check_vma=False)
```

```python
import functools

import jax
import jax.numpy as jnp
from jax import lax
from jax.experimental import pallas as pl
from jax.experimental.pallas import tpu as pltpu
from jax.sharding import PartitionSpec as P


BLK = 128
trace_decay = 0.998
epsilon = 1e-05
OUTSIDE = 1e30
ROWS = 8


def column(ref, first, dtype):
    row = lax.broadcasted_iota(jnp.int32, (ROWS, BLK), 0)
    out = jnp.zeros((ROWS, BLK), dtype)
    for k in range(ROWS):
        out = jnp.where(row == k, ref[first + k], out)
    return out[:, :1]


def advantage_kernel(
    horizon_hbm, lengths_hbm, rewards_hbm, values_hbm,
    returns_ref, blocks_ref, moments_ref,
    horizon_ref, lengths_ref, rewards_ref, values_ref, sems,
):
    seqs, local = rewards_ref.shape
    per_row = local // BLK
    small = [
        pltpu.make_async_copy(horizon_hbm, horizon_ref, sems.at[0]),
        pltpu.make_async_copy(lengths_hbm, lengths_ref, sems.at[1]),
    ]
    large = []
    for k in range(seqs // ROWS):
        rows = pl.ds(k * ROWS, ROWS)
        large.append(pltpu.make_async_copy(values_hbm.at[rows, :], values_ref.at[rows, :], sems.at[2 + 2 * k]))
        large.append(pltpu.make_async_copy(rewards_hbm.at[rows, :], rewards_ref.at[rows, :], sems.at[3 + 2 * k]))
    for copy in small + large:
        copy.start()
    for copy in small:
        copy.wait()
    lane = lax.broadcasted_iota(jnp.int32, (ROWS, BLK), 1)
    count = 0
    for k in range(seqs):
        count = count + lengths_ref[k]
    count = jnp.full((1, 1), count.astype(jnp.float32), jnp.float32)
    sums = jnp.zeros((ROWS, BLK), jnp.float32)
    for first in range(0, seqs, ROWS):
        rows = pl.ds(first, ROWS)
        length = column(lengths_ref, first, jnp.int32)
        discount = 1.0 - 1.0 / column(horizon_ref, first, jnp.float32)
        power = discount * trace_decay
        decay = power
        steps, step = [], 1
        while step < BLK:
            steps.append(jnp.where(lane < BLK - step, power, 0.0))
            decay = jnp.where((BLK - 1 - lane) & step != 0, decay * power, decay)
            power = power * power
            step *= 2
        for copy in large[first // ROWS * 2 : first // ROWS * 2 + 2]:
            copy.wait()
        carry = jnp.zeros((ROWS, BLK), jnp.float32)
        after = None
        for block in reversed(range(per_row)):
            at = pl.ds(block * BLK, BLK)
            rewards = rewards_ref[rows, at]
            values = values_ref[rows, at]
            inside = lane < length - block * BLK
            follows = lane + 1 < length - block * BLK
            rolled = pltpu.roll(values, BLK - 1, 1)
            after = rolled if after is None else after
            upcoming = jnp.where(follows, jnp.where(lane < BLK - 1, rolled, after), 0.0)
            after = rolled
            total = jnp.where(inside, rewards + discount * upcoming - values, 0.0)
            for k, weight in enumerate(steps):
                total = total + weight * pltpu.roll(total, BLK - 2**k, 1)
            head = jnp.broadcast_to(total[:, :1], (ROWS, BLK))
            total = total + decay * carry
            carry = head + power * carry
            total = jnp.where(inside, total, 0.0)
            sums = sums + total
            returns_ref[rows, at] = jnp.where(inside, total + values, 0.0)
            blocks_ref[pl.ds(first * per_row + block, ROWS, stride=per_row), :] = jnp.where(inside, total, OUTSIDE)
    mean = jnp.sum(jnp.sum(sums, axis=0, keepdims=True), axis=1, keepdims=True) / count
    squares = jnp.zeros((ROWS, BLK), jnp.float32)
    for k in range(0, blocks_ref.shape[0], ROWS):
        marked = blocks_ref[pl.ds(k, ROWS), :]
        off = jnp.where(marked == OUTSIDE, 0.0, marked - mean)
        squares = squares + off * off
    spread = jnp.sum(jnp.sum(squares, axis=0, keepdims=True), axis=1, keepdims=True)
    row = jnp.where(lane == 0, count, jnp.where(lane == 1, mean, jnp.where(lane == 2, spread, 0.0)))
    for k in range(0, moments_ref.shape[0], ROWS):
        moments_ref[pl.ds(k, ROWS), :] = row


def gather_kernel(members, wanted_hbm, returns_ref, *refs):
    sources, (moved_ref, returns_hbm, pool_ref, wanted_ref, sems) = refs[:members], refs[members:]
    slots = moved_ref.shape[0]
    share = sources[0].shape[0]
    fetch = pltpu.make_async_copy(wanted_hbm, wanted_ref, sems.at[0])
    fetch.start()
    write = pltpu.make_async_copy(returns_ref, returns_hbm, sems.at[1])
    write.start()
    group = lax.axis_index("group")
    for k in range(members):
        owner = lax.rem(group + k, members)
        pool_ref[pl.ds(pl.multiple_of(owner * share, share), share), :] = sources[k][...]
    fetch.wait()

    def move(i, carry):
        first = pl.multiple_of(i * ROWS, ROWS)
        for k in range(ROWS):
            moved_ref[pl.ds(first + k, 1), :] = pool_ref[pl.ds(wanted_ref[0, first + k], 1), :]
        return carry

    lax.fori_loop(0, slots // ROWS, move, 0)
    write.wait()


def whiten_kernel(moments_ref, moved_ref, train_hbm, train_ref, sems):
    moments = moments_ref[...]
    count, mean, spread = moments[:, 0:1], moments[:, 1:2], moments[:, 2:3]
    total = jnp.sum(count, axis=0, keepdims=True)
    center = jnp.sum(count * mean, axis=0, keepdims=True) / total
    deviation = jnp.sum(spread + count * (mean - center) ** 2, axis=0, keepdims=True)
    scale = jnp.broadcast_to(lax.rsqrt(deviation / total + epsilon), (1, BLK))
    center = jnp.broadcast_to(center, (1, BLK))
    pieces = sems.shape[0]
    depth = moved_ref.shape[0] // pieces
    copies = []
    for k in range(pieces):
        rows = pl.ds(k * depth, depth)
        moved = moved_ref[rows, :]
        train_ref[rows, :] = jnp.where(moved == OUTSIDE, 0.0, (moved - center) * scale)
        copies.append(pltpu.make_async_copy(train_ref.at[rows, :], train_hbm.at[rows, :], sems.at[k]))
        copies[-1].start()
    for copy in copies:
        copy.wait()


def in_hbm(array):
    return pltpu.with_memory_space_constraint(array, pltpu.HBM)


def body(rewards, values, horizon, lengths, assignment):
    seqs, local = rewards.shape
    n_dp, n_group = lax.axis_size("dp"), lax.axis_size("group")
    slots = assignment.shape[-1]
    vmem = pl.BlockSpec(memory_space=pltpu.VMEM)
    hbm = pl.BlockSpec(memory_space=pltpu.HBM)
    params = pltpu.CompilerParams(vmem_limit_bytes=16 << 20)
    f32, i32 = jnp.float32, jnp.int32
    share = seqs * local // BLK
    returns, blocks, moments = pl.pallas_call(
        advantage_kernel,
        out_shape=(
            jax.ShapeDtypeStruct((seqs, local), f32),
            jax.ShapeDtypeStruct((share, BLK), f32),
            jax.ShapeDtypeStruct((n_dp * n_group, BLK), f32),
        ),
        in_specs=[hbm, hbm, hbm, hbm],
        out_specs=(vmem, vmem, vmem),
        scratch_shapes=[
            pltpu.SMEM((seqs,), f32),
            pltpu.SMEM((seqs,), i32),
            pltpu.VMEM((seqs, local), f32),
            pltpu.VMEM((seqs, local), f32),
            pltpu.SemaphoreType.DMA((2 + 2 * (seqs // ROWS),)),
        ],
        compiler_params=params,
        name="advantage",
    )(*map(in_hbm, (horizon, lengths, rewards, values)))
    sources = [blocks]
    for k in range(1, n_group):
        sources.append(lax.ppermute(blocks, "group", [((i + k) % n_group, i) for i in range(n_group)]))
    moments = lax.all_to_all(moments, ("dp", "group"), 0, 0, tiled=True)
    moved, returns = pl.pallas_call(
        functools.partial(gather_kernel, n_group),
        out_shape=(jax.ShapeDtypeStruct((slots, BLK), f32), jax.ShapeDtypeStruct((seqs, local), f32)),
        in_specs=[hbm, vmem] + [vmem] * n_group,
        out_specs=(vmem, hbm),
        scratch_shapes=[
            pltpu.VMEM((n_group * share, BLK), f32),
            pltpu.SMEM((1, slots), i32),
            pltpu.SemaphoreType.DMA((2,)),
        ],
        compiler_params=params,
        name="gather",
    )(in_hbm(assignment), returns, *sources)
    train = pl.pallas_call(
        whiten_kernel,
        out_shape=jax.ShapeDtypeStruct((slots, BLK), f32),
        in_specs=[vmem, vmem],
        out_specs=hbm,
        scratch_shapes=[pltpu.VMEM((slots, BLK), f32), pltpu.SemaphoreType.DMA((4,))],
        compiler_params=params,
        name="whiten",
    )(moments, moved)
    return (returns, train)


def solution(mesh):
    in_specs = (
        P(("dp", "group"), None),
        P(("dp", "group"), None),
        P(("dp", "group")),
        P(("dp", "group")),
        P("dp", "group"),
    )
    out_specs = (P(("dp", "group"), None), P(("dp", "group"), None))

    return jax.shard_map(body, mesh=mesh, in_specs=in_specs, out_specs=out_specs, check_vma=False)
```

```python
import functools

import jax
import jax.numpy as jnp
from jax import lax
from jax.experimental import pallas as pl
from jax.experimental.pallas import tpu as pltpu
from jax.sharding import PartitionSpec as P


BLK = 128
trace_decay = 0.998
epsilon = 1e-05
VALUE_SHARE = 1.0 / trace_decay - 1.0
OUTSIDE = 1e30
ROWS = 8


def column(ref, first, dtype):
    row = lax.broadcasted_iota(jnp.int32, (ROWS, BLK), 0)
    out = jnp.zeros((ROWS, BLK), dtype)
    for k in range(ROWS):
        out = jnp.where(row == k, ref[first + k], out)
    return out[:, :1]


def advantage_kernel(
    horizon_hbm, lengths_hbm, rewards_hbm, values_hbm,
    returns_ref, blocks_ref, moments_ref,
    horizon_ref, lengths_ref, rewards_ref, values_ref, sems,
):
    seqs, local = rewards_ref.shape
    per_row = local // BLK
    small = [
        pltpu.make_async_copy(horizon_hbm, horizon_ref, sems.at[0]),
        pltpu.make_async_copy(lengths_hbm, lengths_ref, sems.at[1]),
    ]
    large = []
    for k in range(seqs // ROWS):
        rows = pl.ds(k * ROWS, ROWS)
        large.append(pltpu.make_async_copy(values_hbm.at[rows, :], values_ref.at[rows, :], sems.at[2 + 2 * k]))
        large.append(pltpu.make_async_copy(rewards_hbm.at[rows, :], rewards_ref.at[rows, :], sems.at[3 + 2 * k]))
    for copy in small + large:
        copy.start()
    for copy in small:
        copy.wait()
    lane = lax.broadcasted_iota(jnp.int32, (ROWS, BLK), 1)
    count = 0
    for k in range(seqs):
        count = count + lengths_ref[k]
    count = jnp.full((1, 1), count.astype(jnp.float32), jnp.float32)
    above = lax.broadcasted_iota(jnp.int32, (BLK, 2 * BLK), 0)
    across = lax.broadcasted_iota(jnp.int32, (BLK, 2 * BLK), 1)
    ones = jnp.where((across >= BLK) | (above >= across), 1.0, 0.0).astype(jnp.bfloat16)
    ones = jnp.concatenate([ones] * 3, axis=0)
    sums = jnp.zeros((ROWS, BLK), jnp.float32)
    for first in range(0, seqs, ROWS):
        rows = pl.ds(first, ROWS)
        left = column(lengths_ref, first, jnp.int32) - lane
        power = (1.0 - 1.0 / column(horizon_ref, first, jnp.float32)) * trace_decay
        rise, step = jnp.ones((ROWS, BLK), jnp.float32), 1
        while step < BLK:
            rise = jnp.where(lane & step != 0, rise * power, rise)
            power = power * power
            step *= 2
        fall = 1.0 / rise
        decay = power * fall
        power = jnp.broadcast_to(power, (ROWS, BLK))
        for copy in large[first // ROWS * 2 : first // ROWS * 2 + 2]:
            copy.wait()
        terms = []
        for block in range(per_row):
            at = pl.ds(block * BLK, BLK)
            term = rewards_ref[rows, at] + VALUE_SHARE * values_ref[rows, at]
            terms.append(jnp.where(left > block * BLK, term, 0.0) * rise)
        rest = jnp.concatenate(terms, axis=0)
        split = []
        for k in range(3):
            split.append(rest.astype(jnp.bfloat16))
            if k < 2:
                rest = rest - split[-1].astype(jnp.float32)
        inner = jnp.dot(jnp.concatenate(split, axis=1), ones, preferred_element_type=jnp.float32)
        carry = jnp.zeros((ROWS, BLK), jnp.float32)
        for block in reversed(range(per_row)):
            at = pl.ds(block * BLK, BLK)
            own = slice(block * ROWS, (block + 1) * ROWS)
            inside = left > block * BLK
            total = inner[own, :BLK] * fall + decay * carry
            carry = inner[own, BLK:] + power * carry
            values = values_ref[rows, at]
            result = jnp.where(inside, total - VALUE_SHARE * values, 0.0)
            returns_ref[rows, at] = result
            advantage = result - values
            sums = sums + jnp.where(inside, advantage, 0.0)
            blocks_ref[pl.ds(first * per_row + block, ROWS, stride=per_row), :] = jnp.where(inside, advantage, OUTSIDE)
    mean = jnp.sum(jnp.sum(sums, axis=0, keepdims=True), axis=1, keepdims=True) / count
    squares = jnp.zeros((ROWS, BLK), jnp.float32)
    for k in range(0, blocks_ref.shape[0], ROWS):
        marked = blocks_ref[pl.ds(k, ROWS), :]
        off = jnp.where(marked == OUTSIDE, 0.0, marked - mean)
        squares = squares + off * off
    spread = jnp.sum(jnp.sum(squares, axis=0, keepdims=True), axis=1, keepdims=True)
    row = jnp.where(lane == 0, count, jnp.where(lane == 1, mean, jnp.where(lane == 2, spread, 0.0)))
    for k in range(0, moments_ref.shape[0], ROWS):
        moments_ref[pl.ds(k, ROWS), :] = row


def gather_kernel(members, wanted_hbm, returns_ref, *refs):
    sources, (moved_ref, returns_hbm, pool_ref, wanted_ref, sems) = refs[:members], refs[members:]
    slots = moved_ref.shape[0]
    share = sources[0].shape[0]
    fetch = pltpu.make_async_copy(wanted_hbm, wanted_ref, sems.at[0])
    fetch.start()
    write = pltpu.make_async_copy(returns_ref, returns_hbm, sems.at[1])
    write.start()
    group = lax.axis_index("group")
    for k in range(members):
        owner = lax.rem(group + k, members)
        pool_ref[pl.ds(pl.multiple_of(owner * share, share), share), :] = sources[k][...]
    fetch.wait()

    def move(i, carry):
        first = pl.multiple_of(i * ROWS, ROWS)
        for k in range(ROWS):
            moved_ref[pl.ds(first + k, 1), :] = pool_ref[pl.ds(wanted_ref[0, first + k], 1), :]
        return carry

    lax.fori_loop(0, slots // ROWS, move, 0)
    write.wait()


def whiten_kernel(moments_ref, moved_ref, train_hbm, train_ref, sems):
    moments = moments_ref[...]
    count, mean, spread = moments[:, 0:1], moments[:, 1:2], moments[:, 2:3]
    total = jnp.sum(count, axis=0, keepdims=True)
    center = jnp.sum(count * mean, axis=0, keepdims=True) / total
    deviation = jnp.sum(spread + count * (mean - center) ** 2, axis=0, keepdims=True)
    scale = jnp.broadcast_to(lax.rsqrt(deviation / total + epsilon), (1, BLK))
    center = jnp.broadcast_to(center, (1, BLK))
    pieces = sems.shape[0]
    depth = moved_ref.shape[0] // pieces
    copies = []
    for k in range(pieces):
        rows = pl.ds(k * depth, depth)
        moved = moved_ref[rows, :]
        train_ref[rows, :] = jnp.where(moved == OUTSIDE, 0.0, (moved - center) * scale)
        copies.append(pltpu.make_async_copy(train_ref.at[rows, :], train_hbm.at[rows, :], sems.at[k]))
        copies[-1].start()
    for copy in copies:
        copy.wait()


def in_hbm(array):
    return pltpu.with_memory_space_constraint(array, pltpu.HBM)


def body(rewards, values, horizon, lengths, assignment):
    seqs, local = rewards.shape
    n_dp, n_group = lax.axis_size("dp"), lax.axis_size("group")
    slots = assignment.shape[-1]
    vmem = pl.BlockSpec(memory_space=pltpu.VMEM)
    hbm = pl.BlockSpec(memory_space=pltpu.HBM)
    params = pltpu.CompilerParams(vmem_limit_bytes=16 << 20)
    f32, i32 = jnp.float32, jnp.int32
    share = seqs * local // BLK
    returns, blocks, moments = pl.pallas_call(
        advantage_kernel,
        out_shape=(
            jax.ShapeDtypeStruct((seqs, local), f32),
            jax.ShapeDtypeStruct((share, BLK), f32),
            pltpu.VMEM((n_dp * n_group, BLK), f32),
        ),
        in_specs=[hbm, hbm, hbm, hbm],
        out_specs=(vmem, vmem, vmem),
        scratch_shapes=[
            pltpu.SMEM((seqs,), f32),
            pltpu.SMEM((seqs,), i32),
            pltpu.VMEM((seqs, local), f32),
            pltpu.VMEM((seqs, local), f32),
            pltpu.SemaphoreType.DMA((2 + 2 * (seqs // ROWS),)),
        ],
        compiler_params=params,
        name="advantage",
    )(*map(in_hbm, (horizon, lengths, rewards, values)))
    sources = [blocks]
    for k in range(1, n_group):
        sources.append(lax.ppermute(blocks, "group", [((i + k) % n_group, i) for i in range(n_group)]))
    moments = lax.all_to_all(moments, ("dp", "group"), 0, 0, tiled=True)
    moved, returns = pl.pallas_call(
        functools.partial(gather_kernel, n_group),
        out_shape=(jax.ShapeDtypeStruct((slots, BLK), f32), jax.ShapeDtypeStruct((seqs, local), f32)),
        in_specs=[hbm, vmem] + [vmem] * n_group,
        out_specs=(vmem, hbm),
        scratch_shapes=[
            pltpu.VMEM((n_group * share, BLK), f32),
            pltpu.SMEM((1, slots), i32),
            pltpu.SemaphoreType.DMA((2,)),
        ],
        compiler_params=params,
        name="gather",
    )(in_hbm(assignment), returns, *sources)
    train = pl.pallas_call(
        whiten_kernel,
        out_shape=jax.ShapeDtypeStruct((slots, BLK), f32),
        in_specs=[vmem, vmem],
        out_specs=hbm,
        scratch_shapes=[pltpu.VMEM((slots, BLK), f32), pltpu.SemaphoreType.DMA((4,))],
        compiler_params=params,
        name="whiten",
    )(moments, moved)
    return (returns, train)


def solution(mesh):
    in_specs = (
        P(("dp", "group"), None),
        P(("dp", "group"), None),
        P(("dp", "group")),
        P(("dp", "group")),
        P("dp", "group"),
    )
    out_specs = (P(("dp", "group"), None), P(("dp", "group"), None))

    return jax.shard_map(body, mesh=mesh, in_specs=in_specs, out_specs=out_specs, check_vma=False)
```

```python
import functools

import jax
import jax.numpy as jnp
from jax import lax
from jax.experimental import pallas as pl
from jax.experimental.pallas import tpu as pltpu
from jax.sharding import PartitionSpec as P


BLK = 128
trace_decay = 0.998
epsilon = 1e-05
VALUE_SHARE = 1.0 / trace_decay - 1.0
OUTSIDE = 1e30
ROWS = 8
PART = BLK // 4


def column(ref, first, dtype):
    row = lax.broadcasted_iota(jnp.int32, (ROWS, BLK), 0)
    out = jnp.zeros((ROWS, BLK), dtype)
    for k in range(ROWS):
        out = jnp.where(row == k, ref[first + k], out)
    return out[:, :1]


def whole(tile):
    return jnp.sum(jnp.sum(tile, axis=0, keepdims=True), axis=1, keepdims=True)


def advantage_kernel(
    horizon_hbm, lengths_hbm, rewards_hbm, values_hbm,
    returns_ref, blocks_ref, moments_ref,
    horizon_ref, lengths_ref, rewards_ref, values_ref, sems,
):
    seqs, local = rewards_ref.shape
    per_row = local // BLK
    small = [
        pltpu.make_async_copy(horizon_hbm, horizon_ref, sems.at[0]),
        pltpu.make_async_copy(lengths_hbm, lengths_ref, sems.at[1]),
    ]
    large = [
        pltpu.make_async_copy(values_hbm, values_ref, sems.at[2]),
        pltpu.make_async_copy(rewards_hbm, rewards_ref, sems.at[3]),
    ]
    for copy in small + large:
        copy.start()
    for copy in small:
        copy.wait()
    lane = lax.broadcasted_iota(jnp.int32, (ROWS, BLK), 1)
    count = 0
    for k in range(seqs):
        count = count + lengths_ref[k]
    count = jnp.full((1, 1), count.astype(jnp.float32), jnp.float32)
    above = lax.broadcasted_iota(jnp.int32, (BLK, 2 * BLK), 0)
    across = lax.broadcasted_iota(jnp.int32, (BLK, 2 * BLK), 1)
    ones = jnp.where((across >= BLK) | (above >= across), 1.0, 0.0).astype(jnp.bfloat16)
    ones = jnp.concatenate([ones] * 3, axis=0)
    groups = []
    for first in range(0, seqs, ROWS):
        left = column(lengths_ref, first, jnp.int32) - lane
        power = (1.0 - 1.0 / column(horizon_ref, first, jnp.float32)) * trace_decay
        rise, step = jnp.ones((ROWS, BLK), jnp.float32), 1
        while step < BLK:
            rise = jnp.where(lane & step != 0, rise * power, rise)
            power = power * power
            step *= 2
        groups.append((left, rise, 1.0 / rise, jnp.broadcast_to(power, (ROWS, BLK))))
    for copy in large:
        copy.wait()
    terms = []
    for g, (left, rise, _, _) in enumerate(groups):
        rows = pl.ds(g * ROWS, ROWS)
        for block in range(per_row):
            at = pl.ds(block * BLK, BLK)
            term = rewards_ref[rows, at] + VALUE_SHARE * values_ref[rows, at]
            terms.append(jnp.where(left > block * BLK, term, 0.0) * rise)
    rest = jnp.concatenate(terms, axis=0)
    split = []
    for k in range(3):
        split.append(rest.astype(jnp.bfloat16))
        if k < 2:
            rest = rest - split[-1].astype(jnp.float32)
    inner = jnp.dot(jnp.concatenate(split, axis=1), ones, preferred_element_type=jnp.float32)
    moments = []
    for g, (left, _, fall, power) in enumerate(groups):
        rows = pl.ds(g * ROWS, ROWS)
        carry = sums = jnp.zeros((ROWS, BLK), jnp.float32)
        for block in reversed(range(per_row)):
            at = pl.ds(block * BLK, BLK)
            tile = (g * per_row + block) * ROWS
            inside = left > block * BLK
            values = jnp.where(inside, values_ref[rows, at], 0.0)
            result = fall * (inner[tile : tile + ROWS, :BLK] + carry) - VALUE_SHARE * values
            advantage = result - values
            carry = power * (inner[tile : tile + ROWS, BLK:] + carry)
            sums = sums + advantage
            returns_ref[rows, at] = result
            blocks_ref[pl.ds(tile, ROWS), :] = jnp.where(inside, advantage, OUTSIDE)
        inside = lax.div(jnp.maximum(left, 0) + BLK - 1, BLK).astype(jnp.float32)
        moments.append([inside, sums, sums / jnp.maximum(inside, 1.0)])
    squares = []
    for g, (_, _, middle) in enumerate(moments):
        parts = [jnp.zeros((ROWS, BLK), jnp.float32)] * 4
        for block in range(per_row):
            marked = blocks_ref[pl.ds((g * per_row + block) * ROWS, ROWS), :]
            off = jnp.where(marked == OUTSIDE, 0.0, marked - middle)
            parts = parts[1:] + [parts[0] + off * off]
        squares.append(sum(parts[1:], parts[0]))
    mean = whole(sum(part[1] for part in moments)) / count
    spread = whole(sum(square + part[0] * (part[2] - mean) ** 2 for square, part in zip(squares, moments)))
    row = jnp.where(lane < PART, count, jnp.where(lane < 2 * PART, count * mean, jnp.where(lane < 3 * PART, mean, spread)))
    for k in range(0, moments_ref.shape[0], ROWS):
        moments_ref[pl.ds(k, ROWS), :] = row


def gather_kernel(members, per_row, wanted_hbm, returns_ref, *refs):
    sources, (moved_ref, returns_hbm, pool_ref, wanted_ref, place_ref, sems) = refs[:members], refs[members:]
    slots = moved_ref.shape[0]
    share = sources[0].shape[0]
    fetch = pltpu.make_async_copy(wanted_hbm, wanted_ref, sems.at[0])
    fetch.start()
    write = pltpu.make_async_copy(returns_ref, returns_hbm, sems.at[1])
    write.start()
    group = lax.axis_index("group")
    for k in range(members):
        owner = lax.rem(group + k, members)
        pool_ref[pl.ds(pl.multiple_of(owner * share, share), share), :] = sources[k][...]
    fetch.wait()
    wanted = wanted_ref[...]
    sequence, block = lax.div(wanted, per_row), lax.rem(wanted, per_row)
    wanted_ref[...] = (lax.div(sequence, ROWS) * per_row + block) * ROWS + lax.rem(sequence, ROWS)
    place = pltpu.make_async_copy(wanted_ref, place_ref, sems.at[0])
    place.start()
    place.wait()

    def move(i, carry):
        first = pl.multiple_of(i * ROWS, ROWS)
        for k in range(ROWS):
            moved_ref[pl.ds(first + k, 1), :] = pool_ref[pl.ds(place_ref[0, first + k], 1), :]
        return carry

    lax.fori_loop(0, slots // ROWS, move, 0)
    write.wait()


def whiten_kernel(moments_ref, moved_ref, train_hbm, train_ref, sems):
    moments = moments_ref[...]
    mean, spread = pltpu.roll(moments, 2 * PART, 1), pltpu.roll(moments, PART, 1)
    sums = jnp.sum(moments, axis=0, keepdims=True)
    total = jnp.broadcast_to(sums[:, :1], (1, BLK))
    center = jnp.broadcast_to(sums[:, PART : PART + 1], (1, BLK)) / total
    deviation = jnp.sum(spread + moments * (mean - center) ** 2, axis=0, keepdims=True)
    deviation = jnp.broadcast_to(deviation[:, :1], (1, BLK))
    scale = lax.rsqrt(deviation / total + epsilon)
    pieces = sems.shape[0]
    depth = moved_ref.shape[0] // pieces
    copies = []
    for k in range(pieces):
        rows = pl.ds(k * depth, depth)
        moved = moved_ref[rows, :]
        train_ref[rows, :] = jnp.where(moved == OUTSIDE, 0.0, (moved - center) * scale)
        copies.append(pltpu.make_async_copy(train_ref.at[rows, :], train_hbm.at[rows, :], sems.at[k]))
        copies[-1].start()
    for copy in copies:
        copy.wait()


def in_hbm(array):
    return pltpu.with_memory_space_constraint(array, pltpu.HBM)


def body(rewards, values, horizon, lengths, assignment):
    seqs, local = rewards.shape
    n_dp, n_group = lax.axis_size("dp"), lax.axis_size("group")
    slots = assignment.shape[-1]
    vmem = pl.BlockSpec(memory_space=pltpu.VMEM)
    hbm = pl.BlockSpec(memory_space=pltpu.HBM)
    params = pltpu.CompilerParams(vmem_limit_bytes=16 << 20)
    f32, i32 = jnp.float32, jnp.int32
    share = seqs * local // BLK
    returns, blocks, moments = pl.pallas_call(
        advantage_kernel,
        out_shape=(
            jax.ShapeDtypeStruct((seqs, local), f32),
            jax.ShapeDtypeStruct((share, BLK), f32),
            pltpu.VMEM((n_dp * n_group, BLK), f32),
        ),
        in_specs=[hbm, hbm, hbm, hbm],
        out_specs=(vmem, vmem, vmem),
        scratch_shapes=[
            pltpu.SMEM((seqs,), f32),
            pltpu.SMEM((seqs,), i32),
            pltpu.VMEM((seqs, local), f32),
            pltpu.VMEM((seqs, local), f32),
            pltpu.SemaphoreType.DMA((4,)),
        ],
        compiler_params=params,
        name="advantage",
    )(*map(in_hbm, (horizon, lengths, rewards, values)))
    sources = [blocks]
    for k in range(1, n_group):
        sources.append(lax.ppermute(blocks, "group", [((i + k) % n_group, i) for i in range(n_group)]))
    moments = lax.all_to_all(moments, ("dp", "group"), 0, 0, tiled=True)
    moved, returns = pl.pallas_call(
        functools.partial(gather_kernel, n_group, local // BLK),
        out_shape=(jax.ShapeDtypeStruct((slots, BLK), f32), jax.ShapeDtypeStruct((seqs, local), f32)),
        in_specs=[hbm, vmem] + [vmem] * n_group,
        out_specs=(vmem, hbm),
        scratch_shapes=[
            pltpu.VMEM((n_group * share, BLK), f32),
            pltpu.VMEM((1, slots), i32),
            pltpu.SMEM((1, slots), i32),
            pltpu.SemaphoreType.DMA((2,)),
        ],
        compiler_params=params,
        name="gather",
    )(in_hbm(assignment), returns, *sources)
    train = pl.pallas_call(
        whiten_kernel,
        out_shape=jax.ShapeDtypeStruct((slots, BLK), f32),
        in_specs=[vmem, vmem],
        out_specs=hbm,
        scratch_shapes=[pltpu.VMEM((slots, BLK), f32), pltpu.SemaphoreType.DMA((4,))],
        compiler_params=params,
        name="whiten",
    )(moments, moved)
    return (returns, train)


def solution(mesh):
    in_specs = (
        P(("dp", "group"), None),
        P(("dp", "group"), None),
        P(("dp", "group")),
        P(("dp", "group")),
        P("dp", "group"),
    )
    out_specs = (P(("dp", "group"), None), P(("dp", "group"), None))

    return jax.shard_map(body, mesh=mesh, in_specs=in_specs, out_specs=out_specs, check_vma=False)
```

```python
import functools

import jax
import jax.numpy as jnp
from jax import lax
from jax.experimental import pallas as pl
from jax.experimental.pallas import tpu as pltpu
from jax.sharding import PartitionSpec as P


BLK = 128
trace_decay = 0.998
epsilon = 1e-05
VALUE_SHARE = 1.0 / trace_decay - 1.0
OUTSIDE = 1e30
ROWS = 8
PART = BLK // 4


def column(ref, first, dtype):
    row = lax.broadcasted_iota(jnp.int32, (ROWS, BLK), 0)
    out = jnp.zeros((ROWS, BLK), dtype)
    for k in range(ROWS):
        out = jnp.where(row == k, ref[first + k], out)
    return out[:, :1]


def whole(tile):
    return jnp.sum(jnp.sum(tile, axis=0, keepdims=True), axis=1, keepdims=True)


def thirds(array):
    parts = []
    for k in range(3):
        parts.append(array.astype(jnp.bfloat16))
        if k < 2:
            array = array - parts[-1].astype(jnp.float32)
    return jnp.concatenate(parts, axis=1)


def advantage_kernel(
    horizon_hbm, lengths_hbm, wanted_hbm, rewards_hbm, values_hbm,
    returns_ref, blocks_ref, moments_ref, columns_ref,
    horizon_ref, lengths_ref, wanted_ref, rewards_ref, values_ref, sems,
):
    seqs, local = rewards_ref.shape
    per_row = local // BLK
    small = [
        pltpu.make_async_copy(horizon_hbm, horizon_ref, sems.at[0]),
        pltpu.make_async_copy(lengths_hbm, lengths_ref, sems.at[1]),
    ]
    large = [
        pltpu.make_async_copy(values_hbm, values_ref, sems.at[2]),
        pltpu.make_async_copy(rewards_hbm, rewards_ref, sems.at[3]),
    ]
    fetch = pltpu.make_async_copy(wanted_hbm, wanted_ref, sems.at[4])
    for copy in small + large + [fetch]:
        copy.start()
    for copy in small:
        copy.wait()
    lane = lax.broadcasted_iota(jnp.int32, (ROWS, BLK), 1)
    count = 0
    for k in range(seqs):
        count = count + lengths_ref[k]
    count = jnp.full((1, 1), count.astype(jnp.float32), jnp.float32)
    above = lax.broadcasted_iota(jnp.int32, (BLK, 2 * BLK), 0)
    across = lax.broadcasted_iota(jnp.int32, (BLK, 2 * BLK), 1)
    ones = jnp.where((across >= BLK) | (above >= across), 1.0, 0.0).astype(jnp.bfloat16)
    ones = jnp.concatenate([ones] * 3, axis=0)
    groups = []
    for first in range(0, seqs, ROWS):
        left = column(lengths_ref, first, jnp.int32) - lane
        power = (1.0 - 1.0 / column(horizon_ref, first, jnp.float32)) * trace_decay
        rise, step = jnp.ones((ROWS, BLK), jnp.float32), 1
        while step < BLK:
            rise = jnp.where(lane & step != 0, rise * power, rise)
            power = power * power
            step *= 2
        groups.append((left, rise, 1.0 / rise, jnp.broadcast_to(power, (ROWS, BLK))))
    fetch.wait()
    wanted = wanted_ref[...]
    sequence, block = lax.div(wanted, per_row), lax.rem(wanted, per_row)
    wanted = (lax.div(sequence, ROWS) * per_row + block) * ROWS + lax.rem(sequence, ROWS)
    wanted = wanted.astype(jnp.float32)
    for k in range(0, columns_ref.shape[0], BLK):
        columns_ref[pl.ds(k, BLK), :] = jnp.broadcast_to(wanted[:, k : k + BLK], (BLK, BLK)).T
    for copy in large:
        copy.wait()
    terms = []
    for g, (left, rise, _, _) in enumerate(groups):
        rows = pl.ds(g * ROWS, ROWS)
        for block in range(per_row):
            at = pl.ds(block * BLK, BLK)
            term = rewards_ref[rows, at] + VALUE_SHARE * values_ref[rows, at]
            terms.append(jnp.where(left > block * BLK, term, 0.0) * rise)
    inner = jnp.dot(thirds(jnp.concatenate(terms, axis=0)), ones, preferred_element_type=jnp.float32)
    moments = []
    for g, (left, _, fall, power) in enumerate(groups):
        rows = pl.ds(g * ROWS, ROWS)
        carry = pivot = sums = squares = jnp.zeros((ROWS, BLK), jnp.float32)
        known = left > per_row * BLK
        for block in reversed(range(per_row)):
            at = pl.ds(block * BLK, BLK)
            tile = (g * per_row + block) * ROWS
            inside = left > block * BLK
            values = jnp.where(inside, values_ref[rows, at], 0.0)
            result = fall * (inner[tile : tile + ROWS, :BLK] + carry) - VALUE_SHARE * values
            advantage = result - values
            carry = power * (inner[tile : tile + ROWS, BLK:] + carry)
            pivot = jnp.where(known, pivot, advantage)
            known = inside
            off = advantage - pivot
            sums = sums + off
            squares = squares + off * off
            returns_ref[rows, at] = result
            blocks_ref[pl.ds(tile, ROWS), :] = jnp.where(inside, advantage, OUTSIDE)
        inside = lax.div(jnp.maximum(left, 0) + BLK - 1, BLK).astype(jnp.float32)
        shift = sums / jnp.maximum(inside, 1.0)
        moments.append((inside, pivot + shift, jnp.maximum(squares - sums * shift, 0.0)))
    mean = whole(sum(part[0] * part[1] for part in moments)) / count
    spread = whole(sum(part[2] + part[0] * (part[1] - mean) ** 2 for part in moments))
    row = jnp.where(lane < PART, count, jnp.where(lane < 2 * PART, count * mean, jnp.where(lane < 3 * PART, mean, spread)))
    for k in range(0, moments_ref.shape[0], ROWS):
        moments_ref[pl.ds(k, ROWS), :] = row


def place_kernel(members, moments_ref, columns_ref, returns_ref, *refs):
    sources, (train_hbm, returns_hbm, train_ref, sems) = refs[:members], refs[members:]
    slots = train_ref.shape[0]
    share = sources[0].shape[0]
    pieces = sems.shape[0] - 1
    depth = slots // pieces
    write = pltpu.make_async_copy(returns_ref, returns_hbm, sems.at[pieces])
    write.start()
    group = lax.axis_index("group")
    firsts = [(lax.rem(group + k, members) * share).astype(jnp.float32) for k in range(members)]
    if members == 2 and slots == share:
        place = columns_ref[pl.ds(0, ROWS), :]
        own = (place >= firsts[0]) & (place < firsts[0] + share)
        own = jnp.broadcast_to(own[:1], (share, BLK))
        tables = [jnp.where(own, sources[0][...], sources[1][...])]
        firsts = [jnp.where(own[:1], firsts[0], firsts[1])]
    else:
        tables = [source[...] for source in sources]
    tables = [thirds(table) for table in tables]
    moments = moments_ref[...]
    mean, spread = pltpu.roll(moments, 2 * PART, 1), pltpu.roll(moments, PART, 1)
    sums = jnp.sum(moments, axis=0, keepdims=True)
    total = jnp.broadcast_to(sums[:, :1], (1, BLK))
    center = jnp.broadcast_to(sums[:, PART : PART + 1], (1, BLK)) / total
    deviation = jnp.sum(spread + moments * (mean - center) ** 2, axis=0, keepdims=True)
    deviation = jnp.broadcast_to(deviation[:, :1], (1, BLK))
    scale = lax.rsqrt(deviation / total + epsilon)
    lane = lax.broadcasted_iota(jnp.int32, (depth, BLK), 1).astype(jnp.float32)
    copies = []
    for k in range(pieces):
        rows = pl.ds(k * depth, depth)
        moved = 0.0
        for first, table in zip(firsts, tables):
            place = columns_ref[rows, :] - first - lane
            chosen = [jnp.where(place == at, 1.0, 0.0).astype(jnp.bfloat16) for at in range(0, share, BLK)]
            found = jnp.dot(jnp.concatenate(chosen, axis=1), table, preferred_element_type=jnp.float32)
            moved = moved + (found[:, :BLK] + found[:, BLK : 2 * BLK] + found[:, 2 * BLK :])
        train_ref[rows, :] = jnp.where(moved > 0.5 * OUTSIDE, 0.0, (moved - center) * scale)
        copies.append(pltpu.make_async_copy(train_ref.at[rows, :], train_hbm.at[rows, :], sems.at[k]))
        copies[-1].start()
    for copy in copies + [write]:
        copy.wait()


def in_hbm(array):
    return pltpu.with_memory_space_constraint(array, pltpu.HBM)


def body(rewards, values, horizon, lengths, assignment):
    seqs, local = rewards.shape
    n_dp, n_group = lax.axis_size("dp"), lax.axis_size("group")
    slots = assignment.shape[-1]
    vmem = pl.BlockSpec(memory_space=pltpu.VMEM)
    hbm = pl.BlockSpec(memory_space=pltpu.HBM)
    params = pltpu.CompilerParams(vmem_limit_bytes=16 << 20)
    f32, i32 = jnp.float32, jnp.int32
    share = seqs * local // BLK
    returns, blocks, moments, columns = pl.pallas_call(
        advantage_kernel,
        out_shape=(
            jax.ShapeDtypeStruct((seqs, local), f32),
            jax.ShapeDtypeStruct((share, BLK), f32),
            jax.ShapeDtypeStruct((n_dp * n_group, BLK), f32),
            jax.ShapeDtypeStruct((slots, BLK), f32),
        ),
        in_specs=[hbm] * 5,
        out_specs=(vmem,) * 4,
        scratch_shapes=[
            pltpu.SMEM((seqs,), f32),
            pltpu.SMEM((seqs,), i32),
            pltpu.VMEM((1, slots), i32),
            pltpu.VMEM((seqs, local), f32),
            pltpu.VMEM((seqs, local), f32),
            pltpu.SemaphoreType.DMA((5,)),
        ],
        compiler_params=params,
        name="advantage",
    )(*map(in_hbm, (horizon, lengths, assignment, rewards, values)))
    sources = [blocks]
    for k in range(1, n_group):
        sources.append(lax.ppermute(blocks, "group", [((i + k) % n_group, i) for i in range(n_group)]))
    moments = lax.all_to_all(moments, ("dp", "group"), 0, 0, tiled=True)
    train, returns = pl.pallas_call(
        functools.partial(place_kernel, n_group),
        out_shape=(jax.ShapeDtypeStruct((slots, BLK), f32), jax.ShapeDtypeStruct((seqs, local), f32)),
        in_specs=[vmem, vmem, vmem] + [vmem] * n_group,
        out_specs=(hbm, hbm),
        scratch_shapes=[
            pltpu.VMEM((slots, BLK), f32),
            pltpu.SemaphoreType.DMA((3,)),
        ],
        compiler_params=params,
        name="place",
    )(moments, columns, returns, *sources)
    return (returns, train)


def solution(mesh):
    in_specs = (
        P(("dp", "group"), None),
        P(("dp", "group"), None),
        P(("dp", "group")),
        P(("dp", "group")),
        P("dp", "group"),
    )
    out_specs = (P(("dp", "group"), None), P(("dp", "group"), None))

    return jax.shard_map(body, mesh=mesh, in_specs=in_specs, out_specs=out_specs, check_vma=False)
```
